32 devices in a mesh: dp: 4 (over y, x), expert: 8 (over z, core).
Axes of the slice: x: 2, y: 2, z: 4, core: 2. Of those that a mesh axis runs over, the one named last changes fastest.
Arguments:
- tokens: bfloat16 [1024, 4096], P('dp', 'expert'), may hold values from -6 to 6
- routing: int32 [1024, 2], P('dp'), may hold values from 0 to 3, all different within a row; in each aligned block of 256 rows (0 to 255, 256 to 511, ...) at most 192 rows name the same one
- gate_weight: bfloat16 [4096, 4], P('expert'), may hold values from -0.09375 to 0.09375
- expert_in: bfloat16 [4, 4096, 8192], P('dp', None, 'expert'), may hold values from -0.09375 to 0.09375
- expert_out: bfloat16 [4, 8192, 4096], P('dp', 'expert'), may hold values from -0.75 to 0.75
Outputs:
- mixed: bfloat16 [1024, 4096], P('dp', 'expert')
The draws below stay inside these ranges and needn't reach their ends.
Inputs may be any that keep to these rules, and one draw needn't show every extreme that they name: `routing`: each row names two different experts. Within the 256 rows of one group, no expert is named by more than 192 rows, a bound that some block reaches.
All inputs are finite; a program needn't handle non-finite values.
Results may differ from the reference program's by a relative error of at most 0.02.
Values may be sent and summed in bfloat16 or wider, within the bound.
A program may use at most 64 MiB of HBM per device.

```python
import math
import jax
import jax.numpy as jnp
import numpy as np
from jax import lax

D = 4096
FF = 8192
GROUP = 256
EXPERTS = 4
CAP = 192
TOKENS = 1024
N_DP = 4
N_EXPERT = 8


def strengthened(result, rng, source, target, blocks, factor):
    owner, partner = [(jnp.arange(result.shape[position]) // (result.shape[position] // blocks)).reshape([-1 if axis == position else 1 for axis in range(result.ndim)]) for position in (source, target)]
    chosen = jax.random.permutation(rng, blocks)[partner]
    strong = (owner == chosen) | (owner == (partner + blocks // 2) % blocks)
    return jnp.where(strong, factor * result, result)


def shard_levels(rng, shape, pieces, low, high):
    def one(position, blocks):
        heights = jax.random.uniform(jax.random.fold_in(jax.random.fold_in(rng, 6), position), (blocks,), jnp.float32, low / len(pieces), high / len(pieces))
        return jnp.repeat(jnp.exp(heights), shape[position] // blocks).reshape((-1,) + (1,) * (len(shape) - position - 1))

    factor_of = one(*pieces[0])
    for cut in pieces[1:]:
        factor_of = factor_of * one(*cut)
    return factor_of


def assign_block(stream_key, own, number, rows, count, top, bound, slope):
    sequence = jax.random.permutation(stream_key, count)
    crowded, ordinary = portions_of(count, rows * top, bound, slope, True), portions_of(count, rows * top, bound, slope, False)
    places = jnp.arange(count)

    def named(sizes, turn):
        used = int((sizes > 0).sum())
        fixed = max(1, used // 4)
        passed = fixed + (places - fixed + turn * (used - fixed)) % max(1, count - fixed)
        return jnp.zeros((count,), jnp.int32).at[sequence[jnp.where(places < fixed, places, passed)]].set(jnp.asarray(sizes, jnp.int32))

    sizes = jnp.where(number % 4 == 0, named(crowded, number // 4), named(ordinary, number - number // 4 - 1))
    mixed = jax.random.permutation(jax.random.fold_in(own, 3), count)
    donor, sink = mixed[0:count // 2 * 2:2], mixed[1:count // 2 * 2:2]
    room = jnp.minimum(sizes[donor] - 1, bound - sizes[sink]) // 2
    room = jnp.where((donor == sequence[0]) | (sink == sequence[0]) | (sizes[sink] == 0), 0, jnp.maximum(room, 0))
    passed = jax.random.randint(jax.random.fold_in(own, 4), (count // 2,), 0, 1 << 20) % (room + 1)
    sizes = sizes.at[donor].add(-passed).at[sink].add(passed)
    items = jnp.searchsorted(jnp.cumsum(sizes), jnp.arange(rows * top), side="right").astype(jnp.int32)
    table = items.reshape(top, rows).T
    table = table[jax.random.permutation(jax.random.fold_in(own, 1), rows)]
    turn = jax.random.randint(jax.random.fold_in(own, 2), (rows, 1), 0, top)
    return jnp.take_along_axis(table, (jnp.arange(top)[None, :] + turn) % top, axis=1)


def portions_of(count, total, most, slope, full):
    weights = [(1 << 20) // math.isqrt(grade ** slope) + 1 for grade in range(1, count + 1)]
    largest = most if full else min(most, max(-(-total // count), total * weights[0] // sum(weights)))
    least = 1 if total - largest >= count - 1 else 0
    counts, surplus = [largest] + [least] * (count - 1), total - largest - least * (count - 1)
    while surplus > 0:
        candidates = [i for i in range(1, count) if counts[i] < largest] or [i for i in range(1, count) if counts[i] < most]
        whole, left = sum([weights[i] for i in candidates]), surplus
        for i in candidates:
            more = min(most - counts[i], max(1, left * weights[i] // whole), surplus)
            counts[i] = counts[i] + more
            surplus = surplus - more
    return np.array(counts)


def centred(rng, dims, deviation, most, shards=(), kind=jnp.bfloat16):
    result = deviation * jax.random.normal(rng, dims, jnp.float32)
    if shards:
        result = result * shard_levels(rng, dims, shards, -0.22, 0.18)
    return jnp.clip(result, -most, most).astype(kind)


def noise_with(key, shape, deviation, bound, shards, heavy, kind=jnp.bfloat16):
    array = deviation * jax.random.normal(key, shape, jnp.float32)
    if shards:
        array = array * shard_levels(key, shape, shards, -0.22, 0.18)
    return jnp.clip(strengthened(array, jax.random.fold_in(key, 3), *heavy), -bound, bound).astype(kind)


def setup_inputs(seed: int = 0) -> dict:
    streams_of = jax.random.split(jax.random.key(seed), 6)
    tokens = centred(streams_of[0], (TOKENS, D), 1.0, 6.0, ((0, 4), (1, 8)))
    routing_keys = jax.random.split(jax.random.fold_in(streams_of[1], 1), TOKENS // GROUP)
    routing_turns = jax.random.permutation(jax.random.fold_in(streams_of[1], 3), TOKENS // GROUP)
    routing = jax.vmap(lambda own, number: assign_block(jax.random.fold_in(streams_of[1], 2), own, number, GROUP, EXPERTS, 2, CAP, 2))(routing_keys, routing_turns).reshape((TOKENS, 2))
    gate_weight = centred(streams_of[2], (D, EXPERTS), D ** -0.5, 0.09375, ((0, 8),))
    expert_in = centred(streams_of[3], (EXPERTS, D, FF), D ** -0.5, 0.09375, ((0, 4), (2, 8)))
    expert_out = noise_with(streams_of[4], (EXPERTS, FF, D), (FF // 64) ** -0.5, 0.75, ((0, 4), (1, 8)), (1, 2, 8, 2.0))
    return {"tokens": tokens, "routing": routing, "gate_weight": gate_weight, "expert_in": expert_in, "expert_out": expert_out}


def slot_table(grouped):
    order = jnp.transpose(grouped, (0, 2, 1)).reshape(grouped.shape[0], -1)
    onehot = (order[:, :, None] == jnp.arange(EXPERTS, dtype=jnp.int32)[None, None, :]).astype(jnp.int32)
    before = jnp.cumsum(onehot, axis=1) - onehot
    slot_flat = jnp.sum(before * onehot, axis=-1).astype(jnp.int32)
    return jnp.transpose(slot_flat.reshape(grouped.shape[0], 2, -1), (0, 2, 1))


def reference(tokens, routing, gate_weight, expert_in, expert_out):
    logits = jnp.dot(tokens, gate_weight, preferred_element_type=jnp.float32)
    raised = jnp.exp(logits)
    softmax_all = raised / jnp.sum(raised, axis=-1, keepdims=True)
    chosen = jnp.take_along_axis(softmax_all, routing, axis=1).astype(jnp.bfloat16)
    grouped = routing.reshape(N_DP, GROUP, 2)
    slot_index = slot_table(grouped)
    group_ids = jnp.broadcast_to(jnp.arange(N_DP, dtype=jnp.int32)[:, None, None], (N_DP, GROUP, 2))
    token_rows = jnp.broadcast_to(tokens.reshape(N_DP, GROUP, 1, D), (N_DP, GROUP, 2, D))
    buffer = jnp.zeros((EXPERTS, N_DP, CAP, D), jnp.bfloat16)
    buffer = buffer.at[grouped, group_ids, slot_index].set(token_rows)
    width_block = FF // N_EXPERT

    def run_expert(packed):
        rows_in, weight_in, weight_out = packed
        flat_rows = rows_in.reshape(N_DP * CAP, D)
        hidden = jax.nn.gelu(jnp.dot(flat_rows, weight_in, preferred_element_type=jnp.float32), approximate=True).astype(jnp.bfloat16)

        def add_block(index, running):
            start = (index * width_block).astype(jnp.int32)
            left = lax.dynamic_slice_in_dim(hidden, start, width_block, 1)
            right = lax.dynamic_slice_in_dim(weight_out, start, width_block, 0)
            term = jnp.dot(left, right, preferred_element_type=jnp.float32).astype(jnp.bfloat16)
            term = lax.optimization_barrier(term)
            return running + term.astype(jnp.float32)

        summed = lax.fori_loop(0, N_EXPERT, add_block, jnp.zeros((N_DP * CAP, D), jnp.float32))
        return summed.astype(jnp.bfloat16).reshape(N_DP, CAP, D)

    expert_result = lax.map(run_expert, (buffer, expert_in, expert_out))
    picked = expert_result[grouped, group_ids, slot_index]
    weights = chosen.reshape(N_DP, GROUP, 2, 1).astype(jnp.float32)
    mixed = jnp.sum(picked.astype(jnp.float32) * weights, axis=2)
    return mixed.reshape(TOKENS, D).astype(jnp.bfloat16)
```

```python
import functools

import jax
import jax.numpy as jnp
from jax import lax
from jax.experimental import pallas as pl
from jax.experimental.pallas import tpu as pltpu
from jax.sharding import PartitionSpec as P


def softmax_rows(logits):
    raised = jnp.exp(logits)
    return raised / jnp.sum(raised, axis=-1, keepdims=True)


def pick_chosen(softmax_all, picks):
    experts = softmax_all.shape[1]
    labels = lax.broadcasted_iota(jnp.int32, (picks.shape[0], 2, experts), 2)
    selected = labels == picks[:, :, None]
    return jnp.sum(jnp.where(selected, softmax_all[:, None, :], 0.0), axis=-1).astype(jnp.bfloat16)


def expert_rows(block_rows, weight_in, weight_out):
    sources = block_rows.shape[0]
    slots_here = block_rows.shape[1]
    width_local = block_rows.shape[2]
    flat_rows = block_rows.reshape(sources * slots_here, width_local)
    pre_act = jnp.dot(
        lax.all_gather(flat_rows, "expert", axis=1, tiled=True),
        weight_in,
        preferred_element_type=jnp.float32,
    )
    hidden = jax.nn.gelu(pre_act, approximate=True).astype(jnp.bfloat16)
    partial_out = jnp.dot(hidden, weight_out, preferred_element_type=jnp.float32)
    summed = lax.psum_scatter(
        partial_out.astype(jnp.bfloat16), "expert", scatter_dimension=1, tiled=True
    )
    return summed.reshape(sources, slots_here, width_local)


def slots_plan(tokens, routing, gate_weight, expert_in, expert_out):
    group_size = tokens.shape[0]
    width_local = tokens.shape[1]
    experts = gate_weight.shape[1]
    dp_count = lax.axis_size("dp")
    capacity = 3 * group_size // dp_count
    weight_in = expert_in[0]
    weight_out = expert_out[0]
    partial_logits = jnp.dot(tokens, gate_weight, preferred_element_type=jnp.float32)
    logits = lax.psum(partial_logits, "expert")
    chosen = pick_chosen(softmax_rows(logits), routing)
    order = jnp.concatenate([routing[:, 0], routing[:, 1]], axis=0)
    labels = lax.broadcasted_iota(jnp.int32, (2 * group_size, experts), 1)
    onehot = (labels == order[:, None]).astype(jnp.int32)
    before = jnp.cumsum(onehot, axis=0) - onehot
    slot_flat = jnp.sum(before * onehot, axis=1)
    slot_index = jnp.stack([slot_flat[:group_size], slot_flat[group_size:]], axis=1)
    target = routing * capacity + slot_index
    columns = lax.broadcasted_iota(jnp.int32, (group_size, experts * capacity), 1)
    first_hit = columns == target[:, 0:1]
    second_hit = columns == target[:, 1:2]
    assign = jnp.logical_or(first_hit, second_hit).astype(jnp.bfloat16)
    outgoing = jnp.einsum("gs,gd->sd", assign, tokens, preferred_element_type=jnp.float32)
    outgoing = outgoing.astype(jnp.bfloat16).reshape(experts, capacity, width_local)
    incoming = lax.all_to_all(outgoing, "dp", split_axis=0, concat_axis=0, tiled=True)
    processed = expert_rows(incoming, weight_in, weight_out)
    returned_rows = lax.all_to_all(processed, "dp", split_axis=0, concat_axis=0, tiled=True)
    zero_weight = jnp.zeros((), jnp.bfloat16)
    combine = jnp.where(first_hit, chosen[:, 0:1], zero_weight) + jnp.where(
        second_hit, chosen[:, 1:2], zero_weight
    )
    mixed = jnp.dot(
        combine,
        returned_rows.reshape(experts * capacity, width_local),
        preferred_element_type=jnp.float32,
    )
    return mixed.astype(jnp.bfloat16)


MESH = pl.DeviceIdType.MESH
F32 = jnp.float32
BF16 = jnp.bfloat16


def whole_kernel(
    experts,
    tok, extra, win_hbm, wout_hbm, out,
    xs, ex, win, wout, pre, logit, hidden, give, take, part, hop, zin,
    wsem, xs_s, xs_r, zs, zr, fs, fr, ds, dr, es, er, ps, pr, hs, hr, us, ur,
):
    dp, me = lax.axis_index("dp"), lax.axis_index("expert")
    z, k = me // 2, me % 2
    depth = lax.axis_size("expert") // 2
    group, width = tok.shape
    half = group // 2
    gx, gy = dp // 2 * 2 + 1 - dp % 2, (1 - dp // 2) * 2 + dp % 2
    gd = 3 - dp
    other = z * 2 + 1 - k
    top, low = pl.ds(0, half), pl.ds(half, half)
    peers = [(g, me) for g in (gx, gy, gd)]
    peers += [(dp, lax.rem(me + i, 2 * depth)) for i in range(1, 2 * depth)]

    def send(src, dst, s_sem, r_sem, who):
        copy = pltpu.make_async_remote_copy(src, dst, s_sem, r_sem, device_id=who, device_id_type=MESH)
        copy.start()
        started.append(copy)

    def got(ref, s_sem, r_sem):
        pltpu.make_async_remote_copy(ref, ref, s_sem, r_sem, device_id=(dp, other), device_id_type=MESH).wait_recv()

    started = []
    load_in = pltpu.make_async_copy(win_hbm.at[0], win, wsem.at[0])
    load_out = pltpu.make_async_copy(wout_hbm.at[0], wout, wsem.at[1])
    load_in.start()
    load_out.start()
    barrier = pltpu.get_barrier_semaphore()
    for who in peers:
        pl.semaphore_signal(barrier, inc=1, device_id=who, device_id_type=MESH)
    pl.semaphore_wait(barrier, len(peers))

    def origin(s):
        return lax.rem(z + depth - s, depth)

    def spread(s):
        zz = origin(s)
        block = tok if s == 0 else xs.at[dp, zz, k]
        for i, (who, rows) in enumerate(((gx, top), (gy, low), (gx, low), (gy, top))):
            send(block.at[rows], xs.at[dp, zz, k, rows], xs_s.at[s, i], xs_r.at[s, i], (who, me))
        send(block, xs.at[dp, zz, k], ds.at[s, 0], dr.at[s, 0], (dp, other))

    for i in range(1, depth):
        send(tok, xs.at[dp, z, k], zs.at[i], zr.at[i], (dp, lax.rem(z + i, depth) * 2 + k))
    spread(0)
    for i, who in enumerate(peers):
        slot = dp if i < 3 else 4 + i - 3
        send(extra, ex.at[slot], es.at[i], er.at[i], who)
    xs[dp, z, k] = tok[...]
    pre[...] = jnp.zeros_like(pre)
    logit[...] = jnp.zeros_like(logit)
    for i, g in enumerate((gx, gy, gd)):
        got(ex.at[g], es.at[i], er.at[i])
    for i in range(1, 2 * depth):
        got(ex.at[3 + i], es.at[2 + i], er.at[2 + i])
    ex[dp] = extra[...]
    ex[4 + 2 * depth - 1] = extra[...]
    load_in.wait()

    for s in range(depth):
        zz = origin(s)
        got(xs.at[gx, zz, k, top], xs_s.at[s, 0], xs_r.at[s, 0])
        send(xs.at[gx, zz, k, top], xs.at[gx, zz, k, top], fs.at[s, 0], fr.at[s, 0], (gy, me))
        got(xs.at[gy, zz, k, low], xs_s.at[s, 1], xs_r.at[s, 1])
        send(xs.at[gy, zz, k, low], xs.at[gy, zz, k, low], fs.at[s, 1], fr.at[s, 1], (gx, me))
        if s + 1 < depth:
            got(xs.at[dp, origin(s + 1), k], zs.at[s + 1], zr.at[s + 1])
            spread(s + 1)
        got(xs.at[gx, zz, k, low], xs_s.at[s, 2], xs_r.at[s, 2])
        send(xs.at[gx, zz, k], xs.at[gx, zz, k], ds.at[s, 1], dr.at[s, 1], (dp, other))
        got(xs.at[gy, zz, k, top], xs_s.at[s, 3], xs_r.at[s, 3])
        send(xs.at[gy, zz, k], xs.at[gy, zz, k], ds.at[s, 2], dr.at[s, 2], (dp, other))
        got(xs.at[gd, zz, k, top], fs.at[s, 0], fr.at[s, 0])
        got(xs.at[gd, zz, k, low], fs.at[s, 1], fr.at[s, 1])
        send(xs.at[gd, zz, k], xs.at[gd, zz, k], ds.at[s, 3], dr.at[s, 3], (dp, other))
        for i, g in enumerate((dp, gx, gy, gd)):
            got(xs.at[g, zz, 1 - k], ds.at[s, i], dr.at[s, i])

        def gate_of(kk):
            away = lax.rem(me + 2 * depth - (zz * 2 + kk), 2 * depth)
            return ex[4 + lax.rem(away + 2 * depth - 1, 2 * depth)]

        gates = [gate_of(kk) for kk in range(2)]

        def accumulate(g, carry):
            total, score = pre[g], logit[g]
            for kk in range(2):
                rows = pl.ds(pl.multiple_of((zz * 2 + kk) * width, width), width)
                block = xs[g, zz, kk]
                total += jnp.dot(block, win[rows, :], preferred_element_type=F32)
                score += lax.dot_general(gates[kk], block, (((1,), (1,)), ((), ())), preferred_element_type=F32)
            pre[g] = total
            logit[g] = score
            return carry

        lax.fori_loop(0, 4, accumulate, 0)

    def activate(g, carry):
        score = logit[g]
        row = lax.broadcasted_iota(jnp.int32, score.shape, 0)
        raised = jnp.where(row < experts, jnp.exp(score), 0.0)
        chance = raised / jnp.sum(raised, axis=0, keepdims=True)
        mine = jnp.sum(jnp.where(row == dp, chance, 0.0), axis=0, keepdims=True)
        picks = ex[g][:, :group].astype(F32)
        named = jnp.logical_and(jnp.logical_or(row == experts, row == experts + 1), picks == dp.astype(F32))
        hit = jnp.sum(jnp.where(named, 1.0, 0.0), axis=0, keepdims=True)
        scale = mine.astype(BF16).astype(F32) * hit
        column = jnp.transpose(jnp.broadcast_to(scale, (128, group)))[:, :1]
        acted = jax.nn.gelu(pre[g], approximate=True)
        hidden[g] = (acted * column).astype(BF16)
        return carry

    lax.fori_loop(0, 4, activate, 0)
    load_out.wait()

    def target(s):
        return lax.rem(z + 1 + s, depth)

    def product(g, zz, kk):
        cols = pl.ds(pl.multiple_of((zz * 2 + kk) * width, width), width)
        return jnp.dot(hidden[g], wout[:, cols], preferred_element_type=F32)

    def for_partner(s):
        def one(g, carry):
            give[s, g] = product(g, target(s), 1 - k).astype(BF16)
            return carry

        lax.fori_loop(0, 4, one, 0)
        send(give.at[s], take.at[s], ps.at[s], pr.at[s], (dp, other))

    def own(s):
        got(take.at[s], ps.at[s], pr.at[s])

        def one(g, carry):
            part[s, g] = (product(g, target(s), k) + take[s, g].astype(F32)).astype(BF16)
            return carry

        lax.fori_loop(0, 4, one, 0)

    def first_hop(s):
        for i, (g, rows, who) in enumerate(((gd, top, gx), (gd, low, gy), (gx, top, gx), (gy, low, gy))):
            send(part.at[s, g, rows], hop.at[s, i], hs.at[s, i], hr.at[s, i], (who, me))

    def add(s, g, rows, i):
        part[s, g, rows] = (part[s, g, rows].astype(F32) + hop[s, i].astype(F32)).astype(BF16)

    def second_hop(s):
        got(hop.at[s, 0], hs.at[s, 0], hr.at[s, 0])
        add(s, gy, top, 0)
        send(part.at[s, gy, top], hop.at[s, 4], hs.at[s, 4], hr.at[s, 4], (gy, me))
        got(hop.at[s, 1], hs.at[s, 1], hr.at[s, 1])
        add(s, gx, low, 1)
        send(part.at[s, gx, low], hop.at[s, 5], hs.at[s, 5], hr.at[s, 5], (gx, me))

    def settle(s):
        for i in (2, 3, 4, 5):
            got(hop.at[s, i], hs.at[s, i], hr.at[s, i])
        for rows, a, b in ((top, 2, 4), (low, 3, 5)):
            total = part[s, dp, rows].astype(F32) + hop[s, a].astype(F32) + hop[s, b].astype(F32)
            part[s, dp, rows] = total.astype(BF16)
        if s + 1 < depth:
            send(part.at[s, dp], zin.at[s], us.at[s], ur.at[s], (dp, target(s) * 2 + k))

    for_partner(0)
    for_partner(1)
    own(0)
    first_hop(0)
    for s in range(1, depth):
        if s + 1 < depth:
            for_partner(s + 1)
        own(s)
        second_hop(s - 1)
        first_hop(s)
        if s > 1:
            settle(s - 2)
    second_hop(depth - 1)
    settle(depth - 2)
    settle(depth - 1)
    final = part[depth - 1, dp].astype(F32)
    for s in range(depth - 1):
        got(zin.at[s], us.at[s], ur.at[s])
        final += zin[s].astype(F32)
    out[...] = final.astype(BF16)
    for copy in started:
        copy.wait_send()


def tokens_plan(tokens, routing, gate_weight, expert_in, expert_out):
    group, width = tokens.shape
    nx = lax.axis_size("expert")
    depth = nx // 2
    experts = gate_weight.shape[1]
    model, inner = expert_in.shape[1:]
    extra = jnp.concatenate(
        [
            gate_weight.T,
            jnp.pad(routing.T.astype(BF16), ((0, 0), (0, width - group))),
            jnp.zeros((14 - experts, width), BF16),
        ],
        axis=0,
    )
    half = group // 2
    vmem = pltpu.VMEM
    dma = pltpu.SemaphoreType.DMA
    return pl.pallas_call(
        functools.partial(whole_kernel, experts),
        out_shape=jax.ShapeDtypeStruct((group, width), BF16),
        in_specs=[pl.BlockSpec(memory_space=vmem)] * 2 + [pl.BlockSpec(memory_space=pl.ANY)] * 2,
        out_specs=pl.BlockSpec(memory_space=vmem),
        scratch_shapes=[
            vmem((4, depth, 2, group, width), BF16),
            vmem((4 + nx, 16, width), BF16),
            vmem((model, inner), BF16),
            vmem((inner, model), BF16),
            vmem((4, group, inner), F32),
            vmem((4, 16, group), F32),
            vmem((4, group, inner), BF16),
            vmem((depth, 4, group, width), BF16),
            vmem((depth, 4, group, width), BF16),
            vmem((depth, 4, group, width), BF16),
            vmem((depth, 6, half, width), BF16),
            vmem((depth - 1, group, width), BF16),
            dma((2,)),
            dma((depth, 4)), dma((depth, 4)),
            dma((depth,)), dma((depth,)),
            dma((depth, 2)), dma((depth, 2)),
            dma((depth, 4)), dma((depth, 4)),
            dma((2 + nx,)), dma((2 + nx,)),
            dma((depth,)), dma((depth,)),
            dma((depth, 6)), dma((depth, 6)),
            dma((depth - 1,)), dma((depth - 1,)),
        ],
        compiler_params=pltpu.CompilerParams(
            collective_id=0, has_side_effects=True, vmem_limit_bytes=63 * 1024 * 1024
        ),
    )(tokens, extra, expert_in, expert_out)


def solution(mesh):
    placed = (
        P("dp", "expert"),
        P("dp", None),
        P("expert", None),
        P("dp", None, "expert"),
        P("dp", "expert", None),
    )
    body = tokens_plan if mesh.shape["dp"] == 4 else slots_plan
    return jax.shard_map(
        body, mesh=mesh, in_specs=placed, out_specs=P("dp", "expert"), check_vma=False
    )
```

```python
import functools

import jax
import jax.numpy as jnp
from jax import lax
from jax.experimental import pallas as pl
from jax.experimental.pallas import tpu as pltpu
from jax.sharding import PartitionSpec as P


def softmax_rows(logits):
    raised = jnp.exp(logits)
    return raised / jnp.sum(raised, axis=-1, keepdims=True)


def pick_chosen(softmax_all, picks):
    experts = softmax_all.shape[1]
    labels = lax.broadcasted_iota(jnp.int32, (picks.shape[0], 2, experts), 2)
    selected = labels == picks[:, :, None]
    return jnp.sum(jnp.where(selected, softmax_all[:, None, :], 0.0), axis=-1).astype(jnp.bfloat16)


def expert_rows(block_rows, weight_in, weight_out):
    sources = block_rows.shape[0]
    slots_here = block_rows.shape[1]
    width_local = block_rows.shape[2]
    flat_rows = block_rows.reshape(sources * slots_here, width_local)
    pre_act = jnp.dot(
        lax.all_gather(flat_rows, "expert", axis=1, tiled=True),
        weight_in,
        preferred_element_type=jnp.float32,
    )
    hidden = jax.nn.gelu(pre_act, approximate=True).astype(jnp.bfloat16)
    partial_out = jnp.dot(hidden, weight_out, preferred_element_type=jnp.float32)
    summed = lax.psum_scatter(
        partial_out.astype(jnp.bfloat16), "expert", scatter_dimension=1, tiled=True
    )
    return summed.reshape(sources, slots_here, width_local)


def slots_plan(tokens, routing, gate_weight, expert_in, expert_out):
    group_size = tokens.shape[0]
    width_local = tokens.shape[1]
    experts = gate_weight.shape[1]
    dp_count = lax.axis_size("dp")
    capacity = 3 * group_size // dp_count
    weight_in = expert_in[0]
    weight_out = expert_out[0]
    partial_logits = jnp.dot(tokens, gate_weight, preferred_element_type=jnp.float32)
    logits = lax.psum(partial_logits, "expert")
    chosen = pick_chosen(softmax_rows(logits), routing)
    order = jnp.concatenate([routing[:, 0], routing[:, 1]], axis=0)
    labels = lax.broadcasted_iota(jnp.int32, (2 * group_size, experts), 1)
    onehot = (labels == order[:, None]).astype(jnp.int32)
    before = jnp.cumsum(onehot, axis=0) - onehot
    slot_flat = jnp.sum(before * onehot, axis=1)
    slot_index = jnp.stack([slot_flat[:group_size], slot_flat[group_size:]], axis=1)
    target = routing * capacity + slot_index
    columns = lax.broadcasted_iota(jnp.int32, (group_size, experts * capacity), 1)
    first_hit = columns == target[:, 0:1]
    second_hit = columns == target[:, 1:2]
    assign = jnp.logical_or(first_hit, second_hit).astype(jnp.bfloat16)
    outgoing = jnp.einsum("gs,gd->sd", assign, tokens, preferred_element_type=jnp.float32)
    outgoing = outgoing.astype(jnp.bfloat16).reshape(experts, capacity, width_local)
    incoming = lax.all_to_all(outgoing, "dp", split_axis=0, concat_axis=0, tiled=True)
    processed = expert_rows(incoming, weight_in, weight_out)
    returned_rows = lax.all_to_all(processed, "dp", split_axis=0, concat_axis=0, tiled=True)
    zero_weight = jnp.zeros((), jnp.bfloat16)
    combine = jnp.where(first_hit, chosen[:, 0:1], zero_weight) + jnp.where(
        second_hit, chosen[:, 1:2], zero_weight
    )
    mixed = jnp.dot(
        combine,
        returned_rows.reshape(experts * capacity, width_local),
        preferred_element_type=jnp.float32,
    )
    return mixed.astype(jnp.bfloat16)


MESH = pl.DeviceIdType.MESH
F32 = jnp.float32
BF16 = jnp.bfloat16


def whole_kernel(
    experts,
    tok, extra, win_hbm, wout_hbm, out,
    xs, ex, win, wout, pre, logit, hidden, give, take, part, hop, zin,
    wsem, xs_s, xs_r, zs, zr, fs, fr, ds, dr, es, er, ps, pr, hs, hr, us, ur,
):
    dp, me = lax.axis_index("dp"), lax.axis_index("expert")
    z, k = me // 2, me % 2
    depth = lax.axis_size("expert") // 2
    group, width = tok.shape
    half = group // 2
    gx, gy = dp // 2 * 2 + 1 - dp % 2, (1 - dp // 2) * 2 + dp % 2
    gd = 3 - dp
    other = z * 2 + 1 - k
    top, low = pl.ds(0, half), pl.ds(half, half)
    peers = [(g, me) for g in (gx, gy, gd)]
    peers += [(dp, lax.rem(me + i, 2 * depth)) for i in range(1, 2 * depth)]

    def send(src, dst, s_sem, r_sem, who):
        copy = pltpu.make_async_remote_copy(src, dst, s_sem, r_sem, device_id=who, device_id_type=MESH)
        copy.start()
        started.append(copy)

    def got(ref, s_sem, r_sem):
        pltpu.make_async_remote_copy(ref, ref, s_sem, r_sem, device_id=(dp, other), device_id_type=MESH).wait_recv()

    started = []
    load_in = pltpu.make_async_copy(win_hbm.at[0], win, wsem.at[0])
    load_out = pltpu.make_async_copy(wout_hbm.at[0], wout, wsem.at[1])
    load_in.start()
    load_out.start()
    barrier = pltpu.get_barrier_semaphore()
    for who in peers:
        pl.semaphore_signal(barrier, inc=1, device_id=who, device_id_type=MESH)
    pl.semaphore_wait(barrier, len(peers))

    upper = z // 2
    near = z * (1 - upper) + (depth - 1 - z) * upper
    middle = near == 1

    def origin(s):
        seen = near if s == 0 else 1 - near if s == 1 else s
        return seen * (1 - upper) + (depth - 1 - seen) * upper

    def pass_on(block, b, to, s_sem):
        return pltpu.make_async_remote_copy(
            block, xs.at[dp, b, k], s_sem, zr.at[b], device_id=(dp, to * 2 + k), device_id_type=MESH
        )

    def forward(s):
        b = origin(s)
        block = xs.at[dp, b, k]
        to = jnp.where(b < z, z + 1, z - 1)
        return pass_on(block, b, to, zs.at[s])

    def spread(s):
        zz = origin(s)
        block = tok if s == 0 else xs.at[dp, zz, k]
        for i, (who, rows) in enumerate(((gx, top), (gy, low), (gx, low), (gy, top))):
            send(block.at[rows], xs.at[dp, zz, k, rows], xs_s.at[s, i], xs_r.at[s, i], (who, me))
        send(block, xs.at[dp, zz, k], ds.at[s, 0], dr.at[s, 0], (dp, other))

    send(tok, xs.at[dp, z, k], zs.at[0], zr.at[z], (dp, (z + 1 - 2 * (z % 2)) * 2 + k))
    crossing = pass_on(tok, z, depth - 1 - z, zs.at[depth])

    @pl.when(middle)
    def _():
        crossing.start()

    spread(0)
    for i, who in enumerate(peers):
        slot = dp if i < 3 else 4 + i - 3
        send(extra, ex.at[slot], es.at[i], er.at[i], who)
    xs[dp, z, k] = tok[...]
    pre[...] = jnp.zeros_like(pre)
    logit[...] = jnp.zeros_like(logit)
    for i, g in enumerate((gx, gy, gd)):
        got(ex.at[g], es.at[i], er.at[i])
    for i in range(1, 2 * depth):
        got(ex.at[3 + i], es.at[2 + i], er.at[2 + i])
    ex[dp] = extra[...]
    ex[4 + 2 * depth - 1] = extra[...]
    load_in.wait()

    for s in range(depth):
        zz = origin(s)
        got(xs.at[gx, zz, k, top], xs_s.at[s, 0], xs_r.at[s, 0])
        send(xs.at[gx, zz, k, top], xs.at[gx, zz, k, top], fs.at[s, 0], fr.at[s, 0], (gy, me))
        got(xs.at[gy, zz, k, low], xs_s.at[s, 1], xs_r.at[s, 1])
        send(xs.at[gy, zz, k, low], xs.at[gy, zz, k, low], fs.at[s, 1], fr.at[s, 1], (gx, me))
        if s + 1 < depth:
            later = origin(s + 1)
            got(xs.at[dp, later, k], zs.at[s + 1], zr.at[later])
            onward = forward(s + 1)
            pl.when(middle)(onward.start)
            spread(s + 1)
        got(xs.at[gx, zz, k, low], xs_s.at[s, 2], xs_r.at[s, 2])
        send(xs.at[gx, zz, k], xs.at[gx, zz, k], ds.at[s, 1], dr.at[s, 1], (dp, other))
        got(xs.at[gy, zz, k, top], xs_s.at[s, 3], xs_r.at[s, 3])
        send(xs.at[gy, zz, k], xs.at[gy, zz, k], ds.at[s, 2], dr.at[s, 2], (dp, other))
        got(xs.at[gd, zz, k, top], fs.at[s, 0], fr.at[s, 0])
        got(xs.at[gd, zz, k, low], fs.at[s, 1], fr.at[s, 1])
        send(xs.at[gd, zz, k], xs.at[gd, zz, k], ds.at[s, 3], dr.at[s, 3], (dp, other))
        def gate_of(kk):
            away = lax.rem(me + 2 * depth - (zz * 2 + kk), 2 * depth)
            return ex[4 + lax.rem(away + 2 * depth - 1, 2 * depth)]

        gates = [gate_of(kk) for kk in range(2)]

        def accumulate(g, carry):
            total, score = pre[g], logit[g]
            for kk in range(2):
                rows = pl.ds(pl.multiple_of((zz * 2 + kk) * width, width), width)
                block = xs[g, zz, kk]
                total += jnp.dot(block, win[rows, :], preferred_element_type=F32)
                score += lax.dot_general(gates[kk], block, (((1,), (1,)), ((), ())), preferred_element_type=F32)
            pre[g] = total
            logit[g] = score
            return carry

        if s + 1 < depth:
            for i, g in enumerate((dp, gx, gy, gd)):
                got(xs.at[g, zz, 1 - k], ds.at[s, i], dr.at[s, i])
            lax.fori_loop(0, 4, accumulate, 0)

    def activate(g, carry):
        score = logit[g]
        row = lax.broadcasted_iota(jnp.int32, score.shape, 0)
        raised = jnp.where(row < experts, jnp.exp(score), 0.0)
        chance = raised / jnp.sum(raised, axis=0, keepdims=True)
        mine = jnp.sum(jnp.where(row == dp, chance, 0.0), axis=0, keepdims=True)
        picks = ex[g][:, :group].astype(F32)
        named = jnp.logical_and(jnp.logical_or(row == experts, row == experts + 1), picks == dp.astype(F32))
        hit = jnp.sum(jnp.where(named, 1.0, 0.0), axis=0, keepdims=True)
        scale = mine.astype(BF16).astype(F32) * hit
        column = jnp.transpose(jnp.broadcast_to(scale, (128, group)))[:, :1]
        acted = jax.nn.gelu(pre[g], approximate=True)
        hidden[g] = (acted * column).astype(BF16)
        return carry

    for i, g in enumerate((dp, gx, gy, gd)):
        got(xs.at[g, zz, 1 - k], ds.at[depth - 1, i], dr.at[depth - 1, i])
        accumulate(g, 0)
        activate(g, 0)
    load_out.wait()

    def target(s):
        return lax.rem(z + 1 + s, depth)

    def product(g, zz, kk):
        cols = pl.ds(pl.multiple_of((zz * 2 + kk) * width, width), width)
        return jnp.dot(hidden[g], wout[:, cols], preferred_element_type=F32)

    def for_partner(s):
        def one(g, carry):
            give[s, g] = product(g, target(s), 1 - k).astype(BF16)
            return carry

        lax.fori_loop(0, 4, one, 0)
        send(give.at[s], take.at[s], ps.at[s], pr.at[s], (dp, other))

    def own(s):
        got(take.at[s], ps.at[s], pr.at[s])

        def one(g, carry):
            part[s, g] = (product(g, target(s), k) + take[s, g].astype(F32)).astype(BF16)
            return carry

        lax.fori_loop(0, 4, one, 0)

    def first_hop(s):
        for i, (g, rows, who) in enumerate(((gd, top, gx), (gd, low, gy), (gx, top, gx), (gy, low, gy))):
            send(part.at[s, g, rows], hop.at[s, i], hs.at[s, i], hr.at[s, i], (who, me))

    def add(s, g, rows, i):
        part[s, g, rows] = (part[s, g, rows].astype(F32) + hop[s, i].astype(F32)).astype(BF16)

    def second_hop(s):
        got(hop.at[s, 0], hs.at[s, 0], hr.at[s, 0])
        add(s, gy, top, 0)
        send(part.at[s, gy, top], hop.at[s, 4], hs.at[s, 4], hr.at[s, 4], (gy, me))
        got(hop.at[s, 1], hs.at[s, 1], hr.at[s, 1])
        add(s, gx, low, 1)
        send(part.at[s, gx, low], hop.at[s, 5], hs.at[s, 5], hr.at[s, 5], (gx, me))

    def settle(s):
        for i in (2, 3, 4, 5):
            got(hop.at[s, i], hs.at[s, i], hr.at[s, i])
        for rows, a, b in ((top, 2, 4), (low, 3, 5)):
            total = part[s, dp, rows].astype(F32) + hop[s, a].astype(F32) + hop[s, b].astype(F32)
            part[s, dp, rows] = total.astype(BF16)
        if s + 1 < depth:
            send(part.at[s, dp], zin.at[s], us.at[s], ur.at[s], (dp, target(s) * 2 + k))

    for_partner(0)
    for_partner(1)
    own(0)
    first_hop(0)
    for s in range(1, depth):
        if s + 1 < depth:
            for_partner(s + 1)
        own(s)
        second_hop(s - 1)
        first_hop(s)
        if s > 1:
            settle(s - 2)
    second_hop(depth - 1)
    settle(depth - 2)
    settle(depth - 1)
    final = part[depth - 1, dp].astype(F32)
    for s in range(depth - 1):
        got(zin.at[s], us.at[s], ur.at[s])
        final += zin[s].astype(F32)
    out[...] = final.astype(BF16)
    for copy in started:
        copy.wait_send()

    @pl.when(middle)
    def _():
        crossing.wait_send()
        for s in range(1, depth):
            forward(s).wait_send()


def tokens_plan(tokens, routing, gate_weight, expert_in, expert_out):
    group, width = tokens.shape
    nx = lax.axis_size("expert")
    depth = nx // 2
    experts = gate_weight.shape[1]
    model, inner = expert_in.shape[1:]
    extra = jnp.concatenate(
        [
            gate_weight.T,
            jnp.pad(routing.T.astype(BF16), ((0, 0), (0, width - group))),
            jnp.zeros((14 - experts, width), BF16),
        ],
        axis=0,
    )
    half = group // 2
    vmem = pltpu.VMEM
    dma = pltpu.SemaphoreType.DMA
    return pl.pallas_call(
        functools.partial(whole_kernel, experts),
        out_shape=jax.ShapeDtypeStruct((group, width), BF16),
        in_specs=[pl.BlockSpec(memory_space=vmem)] * 2 + [pl.BlockSpec(memory_space=pl.ANY)] * 2,
        out_specs=pl.BlockSpec(memory_space=vmem),
        scratch_shapes=[
            vmem((4, depth, 2, group, width), BF16),
            vmem((4 + nx, 16, width), BF16),
            vmem((model, inner), BF16),
            vmem((inner, model), BF16),
            vmem((4, group, inner), F32),
            vmem((4, 16, group), F32),
            vmem((4, group, inner), BF16),
            vmem((depth, 4, group, width), BF16),
            vmem((depth, 4, group, width), BF16),
            vmem((depth, 4, group, width), BF16),
            vmem((depth, 6, half, width), BF16),
            vmem((depth - 1, group, width), BF16),
            dma((2,)),
            dma((depth, 4)), dma((depth, 4)),
            dma((depth + 1,)), dma((depth,)),
            dma((depth, 2)), dma((depth, 2)),
            dma((depth, 4)), dma((depth, 4)),
            dma((2 + nx,)), dma((2 + nx,)),
            dma((depth,)), dma((depth,)),
            dma((depth, 6)), dma((depth, 6)),
            dma((depth - 1,)), dma((depth - 1,)),
        ],
        compiler_params=pltpu.CompilerParams(
            collective_id=0, has_side_effects=True, vmem_limit_bytes=63 * 1024 * 1024
        ),
    )(tokens, extra, expert_in, expert_out)


def solution(mesh):
    placed = (
        P("dp", "expert"),
        P("dp", None),
        P("expert", None),
        P("dp", None, "expert"),
        P("dp", "expert", None),
    )
    body = tokens_plan if tuple(mesh.shape.values()) == (4, 8) else slots_plan
    return jax.shard_map(
        body, mesh=mesh, in_specs=placed, out_specs=P("dp", "expert"), check_vma=False
    )
```

```python
import functools

import jax
import jax.numpy as jnp
from jax import lax
from jax.experimental import pallas as pl
from jax.experimental.pallas import tpu as pltpu
from jax.sharding import PartitionSpec as P


def softmax_rows(logits):
    raised = jnp.exp(logits)
    return raised / jnp.sum(raised, axis=-1, keepdims=True)


def pick_chosen(softmax_all, picks):
    experts = softmax_all.shape[1]
    labels = lax.broadcasted_iota(jnp.int32, (picks.shape[0], 2, experts), 2)
    selected = labels == picks[:, :, None]
    return jnp.sum(jnp.where(selected, softmax_all[:, None, :], 0.0), axis=-1).astype(jnp.bfloat16)


def expert_rows(block_rows, weight_in, weight_out):
    sources = block_rows.shape[0]
    slots_here = block_rows.shape[1]
    width_local = block_rows.shape[2]
    flat_rows = block_rows.reshape(sources * slots_here, width_local)
    pre_act = jnp.dot(
        lax.all_gather(flat_rows, "expert", axis=1, tiled=True),
        weight_in,
        preferred_element_type=jnp.float32,
    )
    hidden = jax.nn.gelu(pre_act, approximate=True).astype(jnp.bfloat16)
    partial_out = jnp.dot(hidden, weight_out, preferred_element_type=jnp.float32)
    summed = lax.psum_scatter(
        partial_out.astype(jnp.bfloat16), "expert", scatter_dimension=1, tiled=True
    )
    return summed.reshape(sources, slots_here, width_local)


def slots_plan(tokens, routing, gate_weight, expert_in, expert_out):
    group_size = tokens.shape[0]
    width_local = tokens.shape[1]
    experts = gate_weight.shape[1]
    dp_count = lax.axis_size("dp")
    capacity = 3 * group_size // dp_count
    weight_in = expert_in[0]
    weight_out = expert_out[0]
    partial_logits = jnp.dot(tokens, gate_weight, preferred_element_type=jnp.float32)
    logits = lax.psum(partial_logits, "expert")
    chosen = pick_chosen(softmax_rows(logits), routing)
    order = jnp.concatenate([routing[:, 0], routing[:, 1]], axis=0)
    labels = lax.broadcasted_iota(jnp.int32, (2 * group_size, experts), 1)
    onehot = (labels == order[:, None]).astype(jnp.int32)
    before = jnp.cumsum(onehot, axis=0) - onehot
    slot_flat = jnp.sum(before * onehot, axis=1)
    slot_index = jnp.stack([slot_flat[:group_size], slot_flat[group_size:]], axis=1)
    target = routing * capacity + slot_index
    columns = lax.broadcasted_iota(jnp.int32, (group_size, experts * capacity), 1)
    first_hit = columns == target[:, 0:1]
    second_hit = columns == target[:, 1:2]
    assign = jnp.logical_or(first_hit, second_hit).astype(jnp.bfloat16)
    outgoing = jnp.einsum("gs,gd->sd", assign, tokens, preferred_element_type=jnp.float32)
    outgoing = outgoing.astype(jnp.bfloat16).reshape(experts, capacity, width_local)
    incoming = lax.all_to_all(outgoing, "dp", split_axis=0, concat_axis=0, tiled=True)
    processed = expert_rows(incoming, weight_in, weight_out)
    returned_rows = lax.all_to_all(processed, "dp", split_axis=0, concat_axis=0, tiled=True)
    zero_weight = jnp.zeros((), jnp.bfloat16)
    combine = jnp.where(first_hit, chosen[:, 0:1], zero_weight) + jnp.where(
        second_hit, chosen[:, 1:2], zero_weight
    )
    mixed = jnp.dot(
        combine,
        returned_rows.reshape(experts * capacity, width_local),
        preferred_element_type=jnp.float32,
    )
    return mixed.astype(jnp.bfloat16)


MESH = pl.DeviceIdType.MESH
F32 = jnp.float32
BF16 = jnp.bfloat16


def whole_kernel(
    experts,
    tok, gate_in, routes, win_hbm, wout_hbm, out,
    extra,
    xs, ex, win, wout, pre, logit, hidden, give, take, part, hop, zin,
    wsem, xs_s, xs_r, zs, zr, fs, fr, ds, dr, es, er, ps, pr, hs, hr, us, ur,
):
    dp, me = lax.axis_index("dp"), lax.axis_index("expert")
    z, k = me // 2, me % 2
    depth = lax.axis_size("expert") // 2
    group, width = tok.shape
    half = group // 2
    gx, gy = dp // 2 * 2 + 1 - dp % 2, (1 - dp // 2) * 2 + dp % 2
    gd = 3 - dp
    other = z * 2 + 1 - k
    top, low = pl.ds(0, half), pl.ds(half, half)
    peers = [(g, me) for g in (gx, gy, gd)]
    peers += [(dp, lax.rem(me + i, 2 * depth)) for i in range(1, 2 * depth)]

    def send(src, dst, s_sem, r_sem, who):
        copy = pltpu.make_async_remote_copy(src, dst, s_sem, r_sem, device_id=who, device_id_type=MESH)
        copy.start()
        started.append(copy)

    def got(ref, s_sem, r_sem):
        pltpu.make_async_remote_copy(ref, ref, s_sem, r_sem, device_id=(dp, other), device_id_type=MESH).wait_recv()

    started = []
    load_in = pltpu.make_async_copy(win_hbm.at[0], win, wsem.at[0])
    load_out = pltpu.make_async_copy(wout_hbm.at[0], wout, wsem.at[1])
    load_in.start()
    load_out.start()
    barrier = pltpu.get_barrier_semaphore()
    for who in peers:
        pl.semaphore_signal(barrier, inc=1, device_id=who, device_id_type=MESH)
    pl.semaphore_wait(barrier, len(peers))

    upper = z // 2
    near = z * (1 - upper) + (depth - 1 - z) * upper
    middle = near == 1

    def origin(s):
        seen = near if s == 0 else 1 - near if s == 1 else s
        return seen * (1 - upper) + (depth - 1 - seen) * upper

    def pass_on(block, b, to, s_sem):
        return pltpu.make_async_remote_copy(
            block, xs.at[dp, b, k], s_sem, zr.at[b], device_id=(dp, to * 2 + k), device_id_type=MESH
        )

    def forward(s):
        b = origin(s)
        block = xs.at[dp, b, k]
        to = jnp.where(b < z, z + 1, z - 1)
        return pass_on(block, b, to, zs.at[s])

    def spread(s):
        zz = origin(s)
        block = tok if s == 0 else xs.at[dp, zz, k]
        for i, (who, rows) in enumerate(((gx, top), (gy, low), (gx, low), (gy, top))):
            send(block.at[rows], xs.at[dp, zz, k, rows], xs_s.at[s, i], xs_r.at[s, i], (who, me))
        send(block, xs.at[dp, zz, k], ds.at[s, 0], dr.at[s, 0], (dp, other))

    send(tok, xs.at[dp, z, k], zs.at[0], zr.at[z], (dp, (z + 1 - 2 * (z % 2)) * 2 + k))
    crossing = pass_on(tok, z, depth - 1 - z, zs.at[depth])

    @pl.when(middle)
    def _():
        crossing.start()

    spread(0)
    wide = lax.broadcasted_iota(jnp.int32, (16, experts), 0) == lax.broadcasted_iota(jnp.int32, (16, experts), 1)
    pair = lax.broadcasted_iota(jnp.int32, (16, 2), 0) == lax.broadcasted_iota(jnp.int32, (16, 2), 1) + experts
    across = (((1,), (1,)), ((), ()))
    gate_rows = lax.dot_general(
        jnp.where(wide, 1.0, 0.0).astype(BF16), gate_in[...], across, preferred_element_type=F32
    )
    route_rows = lax.dot_general(
        jnp.where(pair, 1.0, 0.0).astype(BF16), routes[...].astype(F32).astype(BF16), across, preferred_element_type=F32
    )
    extra[...] = gate_rows.astype(BF16)
    extra[:, :group] = (gate_rows[:, :group] + route_rows).astype(BF16)
    for i, who in enumerate(peers):
        slot = dp if i < 3 else 4 + i - 3
        send(extra, ex.at[slot], es.at[i], er.at[i], who)
    xs[dp, z, k] = tok[...]
    pre[...] = jnp.zeros_like(pre)
    logit[...] = jnp.zeros_like(logit)
    for i, g in enumerate((gx, gy, gd)):
        got(ex.at[g], es.at[i], er.at[i])
    for i in range(1, 2 * depth):
        got(ex.at[3 + i], es.at[2 + i], er.at[2 + i])
    ex[dp] = extra[...]
    ex[4 + 2 * depth - 1] = extra[...]
    load_in.wait()

    def along(s):
        b = origin(s)
        got(xs.at[dp, b, k], zs.at[s], zr.at[b])

    def relay(s):
        pl.when(middle)(forward(s).start)

    def accumulate(s, g):
        zz = origin(s)
        total, score = pre[g], logit[g]
        for kk in range(2):
            away = lax.rem(me + 2 * depth - (zz * 2 + kk), 2 * depth)
            gate = ex[4 + lax.rem(away + 2 * depth - 1, 2 * depth)]
            rows = pl.ds(pl.multiple_of((zz * 2 + kk) * width, width), width)
            block = xs[g, zz, kk]
            total += jnp.dot(block, win[rows, :], preferred_element_type=F32)
            score += lax.dot_general(gate, block, (((1,), (1,)), ((), ())), preferred_element_type=F32)
        pre[g] = total
        logit[g] = score

    def absorb(s):
        for i, g in enumerate((dp, gx, gy, gd)):
            got(xs.at[g, origin(s), 1 - k], ds.at[s, i], dr.at[s, i])
        lax.fori_loop(0, 4, lambda g, carry: accumulate(s, g) or carry, 0)

    for s in range(depth):
        zz = origin(s)
        got(xs.at[gx, zz, k, top], xs_s.at[s, 0], xs_r.at[s, 0])
        send(xs.at[gx, zz, k, top], xs.at[gx, zz, k, top], fs.at[s, 0], fr.at[s, 0], (gy, me))
        got(xs.at[gy, zz, k, low], xs_s.at[s, 1], xs_r.at[s, 1])
        send(xs.at[gy, zz, k, low], xs.at[gy, zz, k, low], fs.at[s, 1], fr.at[s, 1], (gx, me))
        if s + 1 < depth:
            if s == 0:
                along(1)
                relay(1)
                pl.when(middle)(lambda: along(2))
                relay(2)
            else:
                pl.when(jnp.logical_not(middle))(functools.partial(along, s + 1))
            if s == 1:
                pl.when(middle)(lambda: along(3))
                relay(3)
            spread(s + 1)
        if s > 0:
            absorb(s - 1)
        got(xs.at[gx, zz, k, low], xs_s.at[s, 2], xs_r.at[s, 2])
        send(xs.at[gx, zz, k], xs.at[gx, zz, k], ds.at[s, 1], dr.at[s, 1], (dp, other))
        got(xs.at[gy, zz, k, top], xs_s.at[s, 3], xs_r.at[s, 3])
        send(xs.at[gy, zz, k], xs.at[gy, zz, k], ds.at[s, 2], dr.at[s, 2], (dp, other))
        got(xs.at[gd, zz, k, top], fs.at[s, 0], fr.at[s, 0])
        got(xs.at[gd, zz, k, low], fs.at[s, 1], fr.at[s, 1])
        send(xs.at[gd, zz, k], xs.at[gd, zz, k], ds.at[s, 3], dr.at[s, 3], (dp, other))

    def activate(g, carry):
        score = logit[g]
        row = lax.broadcasted_iota(jnp.int32, score.shape, 0)
        raised = jnp.where(row < experts, jnp.exp(score), 0.0)
        chance = raised / jnp.sum(raised, axis=0, keepdims=True)
        mine = jnp.sum(jnp.where(row == dp, chance, 0.0), axis=0, keepdims=True)
        picks = ex[g][:, :group].astype(F32)
        named = jnp.logical_and(jnp.logical_or(row == experts, row == experts + 1), picks == dp.astype(F32))
        hit = jnp.sum(jnp.where(named, 1.0, 0.0), axis=0, keepdims=True)
        scale = mine.astype(BF16).astype(F32) * hit
        column = jnp.transpose(jnp.broadcast_to(scale, (128, group)))[:, :1]
        acted = jax.nn.gelu(pre[g], approximate=True)
        hidden[g] = (acted * column).astype(BF16)
        return carry

    def target(s):
        return origin(depth - 1 - s)

    def product(g, zz, kk):
        cols = pl.ds(pl.multiple_of((zz * 2 + kk) * width, width), width)
        return jnp.dot(hidden[g], wout[:, cols], preferred_element_type=F32)

    def lend(s, g):
        give[s, g] = product(g, target(s), 1 - k).astype(BF16)

    def keep(s, g):
        part[s, g] = (product(g, target(s), k) + take[s, g].astype(F32)).astype(BF16)

    def for_partner(s):
        lax.fori_loop(0, 4, lambda g, carry: lend(s, g) or carry, 0)
        send(give.at[s], take.at[s], ps.at[s, 0], pr.at[s, 0], (dp, other))

    def own(s):
        got(take.at[s], ps.at[s, 0], pr.at[s, 0])
        lax.fori_loop(0, 4, lambda g, carry: keep(s, g) or carry, 0)

    hops = ((gd, top, gx), (gd, low, gy), (gx, top, gx), (gy, low, gy))

    def leave(s, i):
        g, rows, who = hops[i]
        send(part.at[s, g, rows], hop.at[s, i], hs.at[s, i], hr.at[s, i], (who, me))

    def add(s, g, rows, i):
        part[s, g, rows] = (part[s, g, rows].astype(F32) + hop[s, i].astype(F32)).astype(BF16)

    def second_hop(s):
        got(hop.at[s, 0], hs.at[s, 0], hr.at[s, 0])
        add(s, gy, top, 0)
        send(part.at[s, gy, top], hop.at[s, 4], hs.at[s, 4], hr.at[s, 4], (gy, me))
        got(hop.at[s, 1], hs.at[s, 1], hr.at[s, 1])
        add(s, gx, low, 1)
        send(part.at[s, gx, low], hop.at[s, 5], hs.at[s, 5], hr.at[s, 5], (gx, me))

    outer = z + 1 - 2 * (z % 2)
    last = depth - 1

    def line(s):
        far = jnp.where(middle, depth - 1 - z, outer) if s < 2 else outer
        slot = jnp.where(middle, last + s, s)
        return pltpu.make_async_remote_copy(
            part.at[s, dp], zin.at[slot], us.at[s], ur.at[slot], device_id=(dp, far * 2 + k), device_id_type=MESH
        )

    def settle(s):
        for i in (2, 3, 4, 5):
            got(hop.at[s, i], hs.at[s, i], hr.at[s, i])
        for rows, a, b in ((top, 2, 4), (low, 3, 5)):
            total = part[s, dp, rows].astype(F32) + hop[s, a].astype(F32) + hop[s, b].astype(F32)
            part[s, dp, rows] = total.astype(BF16)
        if s < last:
            pl.when(jnp.logical_not(middle))(line(s).start)

    def gather_in(slot):
        got(zin.at[slot], us.at[0], ur.at[slot])
        return zin[slot].astype(F32)

    def merge(s):
        @pl.when(middle)
        def _():
            came = gather_in(s if s < 2 else last)
            part[s, dp] = (part[s, dp].astype(F32) + came).astype(BF16)
            line(s).start()

    load_out.wait()
    for i, g in enumerate((dp, gx, gy, gd)):
        got(xs.at[g, zz, 1 - k], ds.at[last, i], dr.at[last, i])
        accumulate(last, g)
        activate(g, 0)
        lend(0, g)
        send(give.at[0, g], take.at[0, g], ps.at[0, i], pr.at[0, i], (dp, other))
    for i, g, ways in ((1, gx, (2,)), (2, gy, (3,)), (3, gd, (0, 1)), (0, dp, ())):
        got(take.at[0, g], ps.at[0, i], pr.at[0, i])
        keep(0, g)
        for way in ways:
            leave(0, way)
    for_partner(1)
    own(1)
    leave(1, 0)
    leave(1, 1)
    for_partner(2)
    for s in range(depth):
        second_hop(s)
        if s < last:
            leave(s + 1, 2)
            leave(s + 1, 3)
        if s + 2 < depth:
            own(s + 2)
            leave(s + 2, 0)
            leave(s + 2, 1)
        if s + 3 < depth:
            for_partner(s + 3)
        if s > 1:
            merge(s - 2)
        if s > 0:
            settle(s - 1)
    merge(last - 1)
    settle(last)

    @pl.when(middle)
    def _():
        final = part[last, dp].astype(F32) + gather_in(2) + gather_in(last + 1)
        out[...] = final.astype(BF16)

    @pl.when(jnp.logical_not(middle))
    def _():
        out[...] = (part[last, dp].astype(F32) + gather_in(last + 2)).astype(BF16)

    for s in range(last):
        line(s).wait_send()
    for copy in started:
        copy.wait_send()

    @pl.when(middle)
    def _():
        crossing.wait_send()
        for s in range(1, depth):
            forward(s).wait_send()


def tokens_plan(tokens, routing, gate_weight, expert_in, expert_out):
    group, width = tokens.shape
    nx = lax.axis_size("expert")
    depth = nx // 2
    experts = gate_weight.shape[1]
    model, inner = expert_in.shape[1:]
    half = group // 2
    vmem = pltpu.VMEM
    dma = pltpu.SemaphoreType.DMA
    return pl.pallas_call(
        functools.partial(whole_kernel, experts),
        out_shape=jax.ShapeDtypeStruct((group, width), BF16),
        in_specs=[pl.BlockSpec(memory_space=vmem)] * 3 + [pl.BlockSpec(memory_space=pl.ANY)] * 2,
        out_specs=pl.BlockSpec(memory_space=vmem),
        scratch_shapes=[
            vmem((16, width), BF16),
            vmem((4, depth, 2, group, width), BF16),
            vmem((4 + nx, 16, width), BF16),
            vmem((model, inner), BF16),
            vmem((inner, model), BF16),
            vmem((4, group, inner), F32),
            vmem((4, 16, group), F32),
            vmem((4, group, inner), BF16),
            vmem((depth, 4, group, width), BF16),
            vmem((depth, 4, group, width), BF16),
            vmem((depth, 4, group, width), BF16),
            vmem((depth, 6, half, width), BF16),
            vmem((depth + 2, group, width), BF16),
            dma((2,)),
            dma((depth, 4)), dma((depth, 4)),
            dma((depth + 1,)), dma((depth,)),
            dma((depth, 2)), dma((depth, 2)),
            dma((depth, 4)), dma((depth, 4)),
            dma((2 + nx,)), dma((2 + nx,)),
            dma((depth, 4)), dma((depth, 4)),
            dma((depth, 6)), dma((depth, 6)),
            dma((depth - 1,)), dma((depth + 2,)),
        ],
        compiler_params=pltpu.CompilerParams(
            collective_id=0, has_side_effects=True, vmem_limit_bytes=63 * 1024 * 1024
        ),
    )(tokens, gate_weight, routing, expert_in, expert_out)


def solution(mesh):
    placed = (
        P("dp", "expert"),
        P("dp", None),
        P("expert", None),
        P("dp", None, "expert"),
        P("dp", "expert", None),
    )
    body = tokens_plan if tuple(mesh.shape.values()) == (4, 8) else slots_plan
    return jax.shard_map(
        body, mesh=mesh, in_specs=placed, out_specs=P("dp", "expert"), check_vma=False
    )
```

```python
import functools

import jax
import jax.numpy as jnp
from jax import lax
from jax.experimental import pallas as pl
from jax.experimental.pallas import tpu as pltpu
from jax.sharding import PartitionSpec as P


def softmax_rows(logits):
    raised = jnp.exp(logits)
    return raised / jnp.sum(raised, axis=-1, keepdims=True)


def pick_chosen(softmax_all, picks):
    experts = softmax_all.shape[1]
    labels = lax.broadcasted_iota(jnp.int32, (picks.shape[0], 2, experts), 2)
    selected = labels == picks[:, :, None]
    return jnp.sum(jnp.where(selected, softmax_all[:, None, :], 0.0), axis=-1).astype(jnp.bfloat16)


def expert_rows(block_rows, weight_in, weight_out):
    sources = block_rows.shape[0]
    slots_here = block_rows.shape[1]
    width_local = block_rows.shape[2]
    flat_rows = block_rows.reshape(sources * slots_here, width_local)
    pre_act = jnp.dot(
        lax.all_gather(flat_rows, "expert", axis=1, tiled=True),
        weight_in,
        preferred_element_type=jnp.float32,
    )
    hidden = jax.nn.gelu(pre_act, approximate=True).astype(jnp.bfloat16)
    partial_out = jnp.dot(hidden, weight_out, preferred_element_type=jnp.float32)
    summed = lax.psum_scatter(
        partial_out.astype(jnp.bfloat16), "expert", scatter_dimension=1, tiled=True
    )
    return summed.reshape(sources, slots_here, width_local)


def slots_plan(tokens, routing, gate_weight, expert_in, expert_out):
    group_size = tokens.shape[0]
    width_local = tokens.shape[1]
    experts = gate_weight.shape[1]
    dp_count = lax.axis_size("dp")
    capacity = 3 * group_size // dp_count
    weight_in = expert_in[0]
    weight_out = expert_out[0]
    partial_logits = jnp.dot(tokens, gate_weight, preferred_element_type=jnp.float32)
    logits = lax.psum(partial_logits, "expert")
    chosen = pick_chosen(softmax_rows(logits), routing)
    order = jnp.concatenate([routing[:, 0], routing[:, 1]], axis=0)
    labels = lax.broadcasted_iota(jnp.int32, (2 * group_size, experts), 1)
    onehot = (labels == order[:, None]).astype(jnp.int32)
    before = jnp.cumsum(onehot, axis=0) - onehot
    slot_flat = jnp.sum(before * onehot, axis=1)
    slot_index = jnp.stack([slot_flat[:group_size], slot_flat[group_size:]], axis=1)
    target = routing * capacity + slot_index
    columns = lax.broadcasted_iota(jnp.int32, (group_size, experts * capacity), 1)
    first_hit = columns == target[:, 0:1]
    second_hit = columns == target[:, 1:2]
    assign = jnp.logical_or(first_hit, second_hit).astype(jnp.bfloat16)
    outgoing = jnp.einsum("gs,gd->sd", assign, tokens, preferred_element_type=jnp.float32)
    outgoing = outgoing.astype(jnp.bfloat16).reshape(experts, capacity, width_local)
    incoming = lax.all_to_all(outgoing, "dp", split_axis=0, concat_axis=0, tiled=True)
    processed = expert_rows(incoming, weight_in, weight_out)
    returned_rows = lax.all_to_all(processed, "dp", split_axis=0, concat_axis=0, tiled=True)
    zero_weight = jnp.zeros((), jnp.bfloat16)
    combine = jnp.where(first_hit, chosen[:, 0:1], zero_weight) + jnp.where(
        second_hit, chosen[:, 1:2], zero_weight
    )
    mixed = jnp.dot(
        combine,
        returned_rows.reshape(experts * capacity, width_local),
        preferred_element_type=jnp.float32,
    )
    return mixed.astype(jnp.bfloat16)


MESH = pl.DeviceIdType.MESH
F32 = jnp.float32
BF16 = jnp.bfloat16


def whole_kernel(
    experts,
    tok, gate_in, routes, win_hbm, wout_hbm, out,
    extra,
    xs, ex, win, wout, pre, logit, hidden, give, take, part, hop, zin,
    wsem, xs_s, xs_r, zs, zr, fs, fr, ds, dr, es, er, ps, pr, hs, hr, us, ur,
):
    dp, me = lax.axis_index("dp"), lax.axis_index("expert")
    z, k = me // 2, me % 2
    depth = lax.axis_size("expert") // 2
    group, width = tok.shape
    half = group // 2
    gx, gy = dp // 2 * 2 + 1 - dp % 2, (1 - dp // 2) * 2 + dp % 2
    gd = 3 - dp
    other = z * 2 + 1 - k
    top, low = pl.ds(0, half), pl.ds(half, half)
    peers = [(g, me) for g in (gx, gy, gd)]
    peers += [(dp, lax.rem(me + i, 2 * depth)) for i in range(1, 2 * depth)]

    def send(src, dst, s_sem, r_sem, who):
        copy = pltpu.make_async_remote_copy(src, dst, s_sem, r_sem, device_id=who, device_id_type=MESH)
        copy.start()
        started.append(copy)

    def got(ref, s_sem, r_sem):
        pltpu.make_async_remote_copy(ref, ref, s_sem, r_sem, device_id=(dp, other), device_id_type=MESH).wait_recv()

    started = []
    load_in = pltpu.make_async_copy(win_hbm.at[0], win, wsem.at[0])
    load_out = pltpu.make_async_copy(wout_hbm.at[0], wout, wsem.at[1])
    load_in.start()
    load_out.start()
    barrier = pltpu.get_barrier_semaphore()
    for who in peers:
        pl.semaphore_signal(barrier, inc=1, device_id=who, device_id_type=MESH)
    pl.semaphore_wait(barrier, len(peers))

    upper = z // 2
    near = z * (1 - upper) + (depth - 1 - z) * upper
    middle = near == 1

    def origin(s):
        seen = near if s == 0 else 1 - near if s == 1 else s
        return seen * (1 - upper) + (depth - 1 - seen) * upper

    def pass_on(block, b, to, s_sem):
        return pltpu.make_async_remote_copy(
            block, xs.at[dp, b, k], s_sem, zr.at[b], device_id=(dp, to * 2 + k), device_id_type=MESH
        )

    def forward(s):
        b = origin(s)
        block = xs.at[dp, b, k]
        to = jnp.where(b < z, z + 1, z - 1)
        return pass_on(block, b, to, zs.at[s])

    def spread(s):
        zz = origin(s)
        block = tok if s == 0 else xs.at[dp, zz, k]
        for i, (who, rows) in enumerate(((gx, top), (gy, low), (gx, low), (gy, top))):
            send(block.at[rows], xs.at[dp, zz, k, rows], xs_s.at[s, i], xs_r.at[s, i], (who, me))
        send(block, xs.at[dp, zz, k], ds.at[s, 0], dr.at[s, 0], (dp, other))

    send(tok, xs.at[dp, z, k], zs.at[0], zr.at[z], (dp, (z + 1 - 2 * (z % 2)) * 2 + k))
    crossing = pass_on(tok, z, depth - 1 - z, zs.at[depth])

    @pl.when(middle)
    def _():
        crossing.start()

    spread(0)
    wide = lax.broadcasted_iota(jnp.int32, (16, experts), 0) == lax.broadcasted_iota(jnp.int32, (16, experts), 1)
    pair = lax.broadcasted_iota(jnp.int32, (16, 2), 0) == lax.broadcasted_iota(jnp.int32, (16, 2), 1) + experts
    across = (((1,), (1,)), ((), ()))
    gate_rows = lax.dot_general(
        jnp.where(wide, 1.0, 0.0).astype(BF16), gate_in[...], across, preferred_element_type=F32
    )
    route_rows = lax.dot_general(
        jnp.where(pair, 1.0, 0.0).astype(BF16), routes[...].astype(F32).astype(BF16), across, preferred_element_type=F32
    )
    extra[...] = gate_rows.astype(BF16)
    extra[:, :group] = (gate_rows[:, :group] + route_rows).astype(BF16)
    for i, who in enumerate(peers):
        slot = dp if i < 3 else 4 + i - 3
        send(extra, ex.at[slot], es.at[i], er.at[i], who)
    xs[dp, z, k] = tok[...]
    pre[...] = jnp.zeros_like(pre)
    logit[...] = jnp.zeros_like(logit)

    def along(s):
        b = origin(s)
        got(xs.at[dp, b, k], zs.at[s], zr.at[b])

    def relay(s):
        pl.when(middle)(forward(s).start)

    def accumulate(s, g):
        zz = origin(s)
        total, score = pre[g], logit[g]
        for kk in range(2):
            away = lax.rem(me + 2 * depth - (zz * 2 + kk), 2 * depth)
            gate = ex[4 + lax.rem(away + 2 * depth - 1, 2 * depth)]
            rows = pl.ds(pl.multiple_of((zz * 2 + kk) * width, width), width)
            block = xs[g, zz, kk]
            total += jnp.dot(block, win[rows, :], preferred_element_type=F32)
            score += lax.dot_general(gate, block, (((1,), (1,)), ((), ())), preferred_element_type=F32)
        pre[g] = total
        logit[g] = score

    def absorb(s):
        for i, g in enumerate((dp, gx, gy, gd)):
            got(xs.at[g, origin(s), 1 - k], ds.at[s, i], dr.at[s, i])
        lax.fori_loop(0, 4, lambda g, carry: accumulate(s, g) or carry, 0)

    for s in range(depth):
        zz = origin(s)
        got(xs.at[gx, zz, k, top], xs_s.at[s, 0], xs_r.at[s, 0])
        send(xs.at[gx, zz, k, top], xs.at[gx, zz, k, top], fs.at[s, 0], fr.at[s, 0], (gy, me))
        got(xs.at[gy, zz, k, low], xs_s.at[s, 1], xs_r.at[s, 1])
        send(xs.at[gy, zz, k, low], xs.at[gy, zz, k, low], fs.at[s, 1], fr.at[s, 1], (gx, me))
        if s + 1 < depth:
            if s == 0:
                along(1)
                relay(1)
                pl.when(middle)(lambda: along(2))
                relay(2)
            else:
                pl.when(jnp.logical_not(middle))(functools.partial(along, s + 1))
            if s == 1:
                pl.when(middle)(lambda: along(3))
                relay(3)
            spread(s + 1)
        if s == 1:
            for i, g in enumerate((gx, gy, gd)):
                got(ex.at[g], es.at[i], er.at[i])
            for i in range(1, 2 * depth):
                got(ex.at[3 + i], es.at[2 + i], er.at[2 + i])
            ex[dp] = extra[...]
            ex[4 + 2 * depth - 1] = extra[...]
            load_in.wait()
        if s > 0:
            absorb(s - 1)
        got(xs.at[gx, zz, k, low], xs_s.at[s, 2], xs_r.at[s, 2])
        send(xs.at[gx, zz, k], xs.at[gx, zz, k], ds.at[s, 1], dr.at[s, 1], (dp, other))
        got(xs.at[gy, zz, k, top], xs_s.at[s, 3], xs_r.at[s, 3])
        send(xs.at[gy, zz, k], xs.at[gy, zz, k], ds.at[s, 2], dr.at[s, 2], (dp, other))
        got(xs.at[gd, zz, k, top], fs.at[s, 0], fr.at[s, 0])
        got(xs.at[gd, zz, k, low], fs.at[s, 1], fr.at[s, 1])
        send(xs.at[gd, zz, k], xs.at[gd, zz, k], ds.at[s, 3], dr.at[s, 3], (dp, other))

    def activate(g, carry):
        score = logit[g]
        row = lax.broadcasted_iota(jnp.int32, score.shape, 0)
        raised = jnp.where(row < experts, jnp.exp(score), 0.0)
        chance = raised / jnp.sum(raised, axis=0, keepdims=True)
        mine = jnp.sum(jnp.where(row == dp, chance, 0.0), axis=0, keepdims=True)
        picks = ex[g][:, :group].astype(F32)
        named = jnp.logical_and(jnp.logical_or(row == experts, row == experts + 1), picks == dp.astype(F32))
        hit = jnp.sum(jnp.where(named, 1.0, 0.0), axis=0, keepdims=True)
        scale = mine.astype(BF16).astype(F32) * hit
        column = jnp.transpose(jnp.broadcast_to(scale, (128, group)))[:, :1]
        acted = jax.nn.gelu(pre[g], approximate=True)
        hidden[g] = (acted * column).astype(BF16)
        return carry

    def target(s):
        return origin(depth - 1 - s)

    def product(g, zz, kk):
        cols = pl.ds(pl.multiple_of((zz * 2 + kk) * width, width), width)
        return jnp.dot(hidden[g], wout[:, cols], preferred_element_type=F32)

    def lend(s, g):
        give[s, g] = product(g, target(s), 1 - k).astype(BF16)

    def keep(s, g):
        part[s, g] = (product(g, target(s), k) + take[s, g].astype(F32)).astype(BF16)

    def for_partner(s):
        lax.fori_loop(0, 4, lambda g, carry: lend(s, g) or carry, 0)
        send(give.at[s], take.at[s], ps.at[s, 0], pr.at[s, 0], (dp, other))

    def own(s):
        got(take.at[s], ps.at[s, 0], pr.at[s, 0])
        lax.fori_loop(0, 4, lambda g, carry: keep(s, g) or carry, 0)

    hops = ((gd, top, gx), (gd, low, gy), (gx, top, gx), (gy, low, gy))

    def leave(s, i):
        g, rows, who = hops[i]
        send(part.at[s, g, rows], hop.at[s, i], hs.at[s, i], hr.at[s, i], (who, me))

    def add(s, g, rows, i):
        part[s, g, rows] = (part[s, g, rows].astype(F32) + hop[s, i].astype(F32)).astype(BF16)

    def second_hop(s):
        got(hop.at[s, 0], hs.at[s, 0], hr.at[s, 0])
        add(s, gy, top, 0)
        send(part.at[s, gy, top], hop.at[s, 4], hs.at[s, 4], hr.at[s, 4], (gy, me))
        got(hop.at[s, 1], hs.at[s, 1], hr.at[s, 1])
        add(s, gx, low, 1)
        send(part.at[s, gx, low], hop.at[s, 5], hs.at[s, 5], hr.at[s, 5], (gx, me))

    outer = z + 1 - 2 * (z % 2)
    last = depth - 1

    def line(s):
        far = jnp.where(middle, depth - 1 - z, outer) if s < 2 else outer
        slot = jnp.where(middle, last + s, s)
        return pltpu.make_async_remote_copy(
            part.at[s, dp], zin.at[slot], us.at[s], ur.at[slot], device_id=(dp, far * 2 + k), device_id_type=MESH
        )

    def settle(s):
        for i in (2, 3, 4, 5):
            got(hop.at[s, i], hs.at[s, i], hr.at[s, i])
        for rows, a, b in ((top, 2, 4), (low, 3, 5)):
            total = part[s, dp, rows].astype(F32) + hop[s, a].astype(F32) + hop[s, b].astype(F32)
            part[s, dp, rows] = total.astype(BF16)
        if s < last:
            pl.when(jnp.logical_not(middle))(line(s).start)

    def gather_in(slot):
        got(zin.at[slot], us.at[0], ur.at[slot])
        return zin[slot].astype(F32)

    def merge(s):
        @pl.when(middle)
        def _():
            came = gather_in(s if s < 2 else last)
            part[s, dp] = (part[s, dp].astype(F32) + came).astype(BF16)
            line(s).start()

    load_out.wait()
    for i, g in enumerate((dp, gx, gy, gd)):
        got(xs.at[g, zz, 1 - k], ds.at[last, i], dr.at[last, i])
        accumulate(last, g)
        activate(g, 0)
        lend(0, g)
        send(give.at[0, g], take.at[0, g], ps.at[0, i], pr.at[0, i], (dp, other))
    for i, g, ways in ((1, gx, (2,)), (2, gy, (3,)), (3, gd, (0, 1)), (0, dp, ())):
        got(take.at[0, g], ps.at[0, i], pr.at[0, i])
        keep(0, g)
        for way in ways:
            leave(0, way)
    for_partner(1)
    own(1)
    leave(1, 0)
    leave(1, 1)
    for_partner(2)
    for s in range(depth):
        second_hop(s)
        if s < last:
            leave(s + 1, 2)
            leave(s + 1, 3)
        if s + 2 < depth:
            own(s + 2)
            leave(s + 2, 0)
            leave(s + 2, 1)
        if s + 3 < depth:
            for_partner(s + 3)
        if s > 1:
            merge(s - 2)
        if s > 0:
            settle(s - 1)
    merge(last - 1)
    settle(last)

    @pl.when(middle)
    def _():
        final = part[last, dp].astype(F32) + gather_in(2) + gather_in(last + 1)
        out[...] = final.astype(BF16)

    @pl.when(jnp.logical_not(middle))
    def _():
        out[...] = (part[last, dp].astype(F32) + gather_in(last + 2)).astype(BF16)

    for s in range(last):
        line(s).wait_send()
    for copy in started:
        copy.wait_send()

    @pl.when(middle)
    def _():
        crossing.wait_send()
        for s in range(1, depth):
            forward(s).wait_send()


def tokens_plan(tokens, routing, gate_weight, expert_in, expert_out):
    group, width = tokens.shape
    nx = lax.axis_size("expert")
    depth = nx // 2
    experts = gate_weight.shape[1]
    model, inner = expert_in.shape[1:]
    half = group // 2
    vmem = pltpu.VMEM
    dma = pltpu.SemaphoreType.DMA
    return pl.pallas_call(
        functools.partial(whole_kernel, experts),
        out_shape=jax.ShapeDtypeStruct((group, width), BF16),
        in_specs=[pl.BlockSpec(memory_space=vmem)] * 3 + [pl.BlockSpec(memory_space=pl.ANY)] * 2,
        out_specs=pl.BlockSpec(memory_space=vmem),
        scratch_shapes=[
            vmem((16, width), BF16),
            vmem((4, depth, 2, group, width), BF16),
            vmem((4 + nx, 16, width), BF16),
            vmem((model, inner), BF16),
            vmem((inner, model), BF16),
            vmem((4, group, inner), F32),
            vmem((4, 16, group), F32),
            vmem((4, group, inner), BF16),
            vmem((depth, 4, group, width), BF16),
            vmem((depth, 4, group, width), BF16),
            vmem((depth, 4, group, width), BF16),
            vmem((depth, 6, half, width), BF16),
            vmem((depth + 2, group, width), BF16),
            dma((2,)),
            dma((depth, 4)), dma((depth, 4)),
            dma((depth + 1,)), dma((depth,)),
            dma((depth, 2)), dma((depth, 2)),
            dma((depth, 4)), dma((depth, 4)),
            dma((2 + nx,)), dma((2 + nx,)),
            dma((depth, 4)), dma((depth, 4)),
            dma((depth, 6)), dma((depth, 6)),
            dma((depth - 1,)), dma((depth + 2,)),
        ],
        compiler_params=pltpu.CompilerParams(
            collective_id=0, has_side_effects=True, vmem_limit_bytes=63 * 1024 * 1024
        ),
    )(tokens, gate_weight, routing, expert_in, expert_out)


def solution(mesh):
    placed = (
        P("dp", "expert"),
        P("dp", None),
        P("expert", None),
        P("dp", None, "expert"),
        P("dp", "expert", None),
    )
    body = tokens_plan if tuple(mesh.shape.values()) == (4, 8) else slots_plan
    return jax.shard_map(
        body, mesh=mesh, in_specs=placed, out_specs=P("dp", "expert"), check_vma=False
    )
```
